1024 devices in a mesh: dp: 64 (over x_lo, z, core), tp: 16 (over y, x_hi).
Axes of the slice: x: 8 (x_hi: 2, x_lo: 4; x = x_hi * 4 + x_lo), y: 8, z: 8, core: 2. Of those that a mesh axis runs over, the one named last changes fastest.
Arguments:
- hidden_states: bfloat16 [16384, 3584], P('dp'), may hold values from -21 to 21
- resp_lengths: int32 [8], replicated, may hold values from 1 to 8448, 16384 in all
- w_query: bfloat16 [3584, 2048], P('dp', 'tp'), may hold values from -0.25 to 0.25
- w_keyval: bfloat16 [3584, 1024], P('dp', 'tp'), may hold values from -0.09375 to 0.09375
- w_out: bfloat16 [2048, 3584], P('tp', 'dp'), may hold values from -0.125 to 0.125
Outputs:
- attended: bfloat16 [16384, 3584], P('dp', 'tp')
The draws below stay inside these ranges and needn't reach their ends.
Inputs may be any that keep to these rules, and one draw needn't show every extreme that they name: `resp_lengths`: the 8 lengths sum to 16384; the longest is exactly 8448.
All inputs are finite; a program needn't handle non-finite values.
Results may differ from the reference program's by a relative error of at most 0.015.
The reference program's roundings to bfloat16 on the way count: a program that leaves them out, or rounds other values in their place, can miss the bound.
Values may be sent and summed in bfloat16 or wider, within the bound.
A program may use at most 64 MiB of HBM per device.

```python
import math
import jax
import jax.numpy as jnp
import numpy as np
from jax import lax

D = 3584
HD = 128
KV = 4
TOK_DEV = 256
HEADS = 16
TOKENS = 16384
LMAX = 8448
NRESP = 8
N_TP = 16


def draw_hidden_states(key, part):
    first_key = jax.random.fold_in(jax.random.fold_in(key, 11), 0)
    values = jnp.clip(jax.random.normal(first_key, (TOKENS, D), jnp.float32), -6.0, 6.0)
    return values.astype(jnp.bfloat16)


def level_of(stream_key, extent, shards, low, high):
    factor_of = 1.0
    for dim, parts in shards:
        draws = jax.random.uniform(jax.random.fold_in(jax.random.fold_in(stream_key, 6), dim), (parts,), jnp.float32, low / len(shards), high / len(shards))
        factor_of = factor_of * jnp.repeat(jnp.exp(draws), extent[dim] // parts).reshape((-1,) + (1,) * (len(extent) - 1 - dim))
    return factor_of


def length_profile(amount, total, reach, slope):
    portions = [(1 << 20) // math.isqrt(grade ** slope) + 1 for grade in range(2, amount + 1)]
    surplus, holding = total - reach - (amount - 1), [1] * (amount - 1)
    while surplus > 0:
        free = [i for i in range(amount - 1) if holding[i] < reach]
        whole, budget = sum([portions[i] for i in free]), surplus
        for i in free:
            extra = min(reach - holding[i], max(1, budget * portions[i] // whole), surplus)
            holding[i] = holding[i] + extra
            surplus = surplus - extra
    return np.array([reach] + holding)


def uneven_parts(own_key, amount, total, limit, skew):
    if amount == 2:
        one = jax.random.randint(own_key, (), max(1, total - limit), min(limit, total - 1) + 1)
        return jnp.stack([one, total - one])
    tallies = jnp.asarray(length_profile(amount, total, limit, skew), jnp.int32)
    couples = (amount - 1) // 2
    donor, sink = tallies[1:1 + 2 * couples:2], tallies[2:2 + 2 * couples:2]
    room = jnp.minimum(donor - 1, limit - sink)
    moved = jax.random.randint(jax.random.fold_in(own_key, 1), (couples,), 0, 1 << 20) % (room + 1)
    tallies = tallies.at[1:1 + 2 * couples:2].set(donor - moved).at[2:2 + 2 * couples:2].set(sink + moved)
    return tallies[jax.random.permutation(jax.random.fold_in(own_key, 2), amount)]


def centred(own_key, shape, width, reach, pieces=(), kind=jnp.bfloat16):
    result = width * jax.random.normal(own_key, shape, jnp.float32)
    if pieces:
        result = result * level_of(own_key, shape, pieces, -0.22, 0.18)
    return jnp.clip(result, -reach, reach).astype(kind)


def setup_inputs(seed: int = 0) -> dict:
    key_list = jax.random.split(jax.random.key(seed), 6)
    hidden_states = draw_hidden_states(jax.random.fold_in(key_list[5], 71), 0)
    resp_lengths = uneven_parts(key_list[1], NRESP, TOKENS, LMAX, 2).astype(jnp.int32)
    w_query = centred(key_list[2], (D, HEADS * HD), (D // 6) ** -0.5, 0.25, ((0, 64), (1, 16)))
    w_keyval = centred(key_list[3], (D, 2 * KV * HD), D ** -0.5, 0.09375, ((0, 64), (1, 16)))
    w_out = centred(key_list[4], (HEADS * HD, D), (HEADS * HD) ** -0.5, 0.125, ((0, 16), (1, 64)))
    return dict(hidden_states=hidden_states, resp_lengths=resp_lengths, w_query=w_query, w_keyval=w_keyval, w_out=w_out)


def reference(hidden_states, resp_lengths, w_query, w_keyval, w_out):
    total_tokens = hidden_states.shape[0]
    head_scale = HD ** -0.5
    query = (jnp.dot(hidden_states, w_query, preferred_element_type=jnp.float32) * head_scale).astype(jnp.bfloat16)
    keyval = jnp.dot(hidden_states, w_keyval, preferred_element_type=jnp.float32).astype(jnp.bfloat16)
    resp_ends = jnp.cumsum(resp_lengths, dtype=jnp.int32)
    position = jnp.arange(total_tokens, dtype=jnp.int32)
    segment = jnp.sum((position[:, None] >= resp_ends[None, :]).astype(jnp.int32), axis=1, dtype=jnp.int32)
    window = min(total_tokens, TOK_DEV + LMAX)
    blocks = total_tokens // TOK_DEV
    per_group = HEADS // KV

    def one_head(head):
        kv_head = (head // per_group).astype(jnp.int32)
        key_head = lax.dynamic_slice_in_dim(keyval, kv_head * HD, HD, 1)
        value_head = lax.dynamic_slice_in_dim(keyval, (KV + kv_head) * HD, HD, 1)
        query_head = lax.dynamic_slice_in_dim(query, (head * HD).astype(jnp.int32), HD, 1)

        def one_block(block):
            begin = (block * TOK_DEV).astype(jnp.int32)
            key_begin = jnp.clip(begin + TOK_DEV - window, 0, total_tokens - window).astype(jnp.int32)
            query_rows = lax.dynamic_slice_in_dim(query_head, begin, TOK_DEV, 0)
            key_rows = lax.dynamic_slice_in_dim(key_head, key_begin, window, 0)
            value_rows = lax.dynamic_slice_in_dim(value_head, key_begin, window, 0)
            query_pos = begin + jnp.arange(TOK_DEV, dtype=jnp.int32)
            key_pos = key_begin + jnp.arange(window, dtype=jnp.int32)
            query_seg = lax.dynamic_slice_in_dim(segment, begin, TOK_DEV, 0)
            key_seg = lax.dynamic_slice_in_dim(segment, key_begin, window, 0)
            scores = jnp.dot(query_rows, key_rows.T, preferred_element_type=jnp.float32)
            allowed = (query_seg[:, None] == key_seg[None, :]) & (key_pos[None, :] <= query_pos[:, None])
            largest = jnp.max(jnp.where(allowed, scores, jnp.float32(-1e30)), axis=1)
            expw = jnp.where(allowed, jnp.exp(scores - largest[:, None]), jnp.float32(0.0))
            denom = jnp.sum(expw, axis=1)
            numer = jnp.dot(expw.astype(jnp.bfloat16), value_rows, preferred_element_type=jnp.float32)
            return (numer / denom[:, None]).astype(jnp.bfloat16)

        return lax.map(one_block, jnp.arange(blocks, dtype=jnp.int32)).reshape(total_tokens, HD)

    heads_all = lax.map(one_head, jnp.arange(HEADS, dtype=jnp.int32))
    heads_out = jnp.transpose(heads_all, (1, 0, 2)).reshape(total_tokens, HEADS * HD)
    group_width = (HEADS // N_TP) * HD
    summed = jnp.zeros((total_tokens, w_out.shape[1]), jnp.float32)
    for group in range(N_TP):
        partial_sum = jnp.dot(heads_out[:, group * group_width:(group + 1) * group_width],
                              w_out[group * group_width:(group + 1) * group_width],
                              preferred_element_type=jnp.float32).astype(jnp.bfloat16)
        partial_sum = lax.optimization_barrier(partial_sum)
        summed = summed + partial_sum.astype(jnp.float32)
    return summed.astype(jnp.bfloat16)
```

```python
import functools

import jax
import jax.numpy as jnp
from jax import lax
from jax.experimental import pallas as pl
from jax.experimental.pallas import tpu as pltpu
from jax.sharding import Mesh
from jax.sharding import PartitionSpec as P

HD = 128
DP = ("dp_0", "dp_1", "dp_2")
TP = ("tp_0", "tp_1")
MESH = pl.DeviceIdType.MESH
F32, BF16 = jnp.float32, jnp.bfloat16
NX, NZ, NC, NY, NH = 4, 8, 2, 8, 2
LOW = -1e30


def wrap(a, n):
    return lax.rem(a + 2 * n, n)


class Book:
    def __init__(self, send, recv):
        self.send, self.recv, self.n_send, self.n_recv, self.open = send, recv, 0, 0, []

    def slot(self, count=1):
        at = self.n_recv
        self.n_recv += count
        return at

    def start(self, src, dst, recv_at, device, pred=None):
        at = self.n_send
        self.n_send += 1
        copy = pltpu.make_async_remote_copy(
            src_ref=src, dst_ref=dst, send_sem=self.send.at[at], recv_sem=self.recv.at[recv_at],
            device_id=device, device_id_type=MESH)
        self.open.append((copy, pred))
        if pred is None:
            copy.start()
        else:
            pl.when(pred)(copy.start)

    def wait(self, dst, recv_at, pred=None):
        copy = pltpu.make_async_remote_copy(
            src_ref=dst, dst_ref=dst, send_sem=self.send.at[0], recv_sem=self.recv.at[recv_at],
            device_id={"dp_2": 1 - lax.axis_index("dp_2")}, device_id_type=MESH)
        if pred is None:
            copy.wait_recv()
        else:
            pl.when(pred)(copy.wait_recv)

    def finish(self):
        for copy, pred in self.open:
            if pred is None:
                copy.wait_send()
            else:
                pl.when(pred)(copy.wait_send)


class Plane:
    def __init__(self, book, buf, pos, up, down):
        self.book, self.buf, self.up, self.down = book, buf, up, down
        self.x, self.z, self.c = pos
        self.rx, self.rup, self.rdown = book.slot(3), book.slot(up), book.slot(down)
        self.rcore = book.slot(up + down + 1)

    def core(self, at, zz):
        ref = self.buf.at[self.c, zz]
        self.book.start(ref, ref, self.rcore + at, {"dp_2": 1 - self.c})

    def x_send(self):
        ref = self.buf.at[self.c, self.z, self.x]
        for d in (1, 2, 3):
            self.book.start(ref, ref, self.rx + d - 1, {"dp_0": wrap(self.x + d, NX)})

    def hop(self, k, step):
        zz = wrap(self.z - step * (k - 1), NZ)
        ref = self.buf.at[self.c, zz]
        base = self.rup if step == 1 else self.rdown
        self.book.start(ref, ref, base + k - 1, {"dp_1": wrap(self.z + step, NZ)})

    def x_wait(self):
        for d in (1, 2, 3):
            self.book.wait(self.buf.at[self.c, self.z, wrap(self.x - d, NX)], self.rx + d - 1)
        self.hop(1, 1)
        self.hop(1, -1)
        self.core(0, self.z)

    def step(self, k):
        for step, last, base, at in ((1, self.up, self.rup, 0), (-1, self.down, self.rdown, self.up)):
            if k <= last:
                zz = wrap(self.z - step * k, NZ)
                self.book.wait(self.buf.at[self.c, zz], base + k - 1)
                if k < last:
                    self.hop(k + 1, step)
                self.core(at + k, zz)

    def core_wait(self):
        for k in range(self.up + 1):
            self.book.wait(self.buf.at[1 - self.c, wrap(self.z - k, NZ)], self.rcore + k)
        for k in range(1, self.down + 1):
            self.book.wait(self.buf.at[1 - self.c, wrap(self.z + k, NZ)], self.rcore + self.up + k)


def received(step, k, row, z):
    if step == 1:
        if row == 0:
            return z >= k
        if row == 1:
            return None if k > 4 else (z >= 0 if k <= 3 else z < 4)
        if k == 1:
            return z >= 0
        if k == 2:
            return (z <= 1) | (z == 7)
        return z <= 2 if k == 3 else None
    if row == 2:
        return z <= 7 - k
    if row == 1:
        return z >= 0 if k <= 3 else z >= 4
    if k == 1:
        return (z == 7) | (z <= 1)
    if k == 2:
        return (z >= 6) | (z == 0)
    return z >= 5 if k == 3 else None


def needed(step, k, row, z):
    if row == 1:
        return received(step, k, row, z)
    if row == 0:
        return (z >= k) if step == 1 else (None if k > 3 else z + k >= 8)
    if step == -1:
        return z <= 7 - k
    if k == 1:
        return z >= 0
    return z < k if k <= 3 else None


def kernel(hid, qstart, wq_in, wx_in, wo_in, out,
           g_q, g_x, g_o, land, w_q, w_x, w_t, qq, made, kv, acc, stat, o_in, stat_in, heads, total,
           send_sem, recv_sem):
    x, z, c = (lax.axis_index(a) for a in DP)
    y, h = (lax.axis_index(a) for a in TP)
    p = lax.rem(y, 2)
    y2 = y + 1 - 2 * p
    book = Book(send_sem, recv_sem)

    y_to = lax.rem(2 * y, NY) + lax.div(y, 4)
    y_from = lax.div(y, 2) + 4 * p
    o_to = (2 * h + lax.rem(z, 2), y, 2 * x + lax.div(z, 4), lax.rem(lax.div(z, 2), 2))
    o_from = (lax.div(y, 2), 4 * p + 2 * h + lax.rem(x, 2), z, lax.div(x, 2))

    def xzyh(t):
        return {"dp_0": t[0], "dp_1": t[1], "tp_0": t[2], "tp_1": t[3]}

    o_self = (o_to[0] == x) & (o_to[1] == z) & (o_to[2] == y) & (o_to[3] == h)
    barrier = pltpu.get_barrier_semaphore()

    def greet(device, own=None):
        def remote():
            pl.semaphore_signal(barrier, inc=1, device_id=device, device_id_type=MESH)

        if own is None:
            remote()
        else:
            pl.when(jnp.logical_not(own))(remote)

    greet(xzyh(o_to), o_self)
    greet(xzyh(o_from), o_self)
    for j in (0, 1):
        greet({"tp_0": y_to, "tp_1": j}, (y_to == y) & (h == j))
        greet({"tp_0": y_from, "tp_1": j}, (y_from == y) & (h == j))
    greet({"dp_0": 3 - x, "dp_1": 7 - z})
    greet({"tp_1": 1 - h})
    for d in (1, 2, 3):
        greet({"dp_0": wrap(x + d, NX)})
    for d in (1, -1):
        greet({"dp_1": wrap(z + d, NZ)})
        greet({"tp_0": wrap(y + d, NY)})
    greet({"tp_0": y2, "dp_2": 1 - c})
    greet({"dp_2": 1 - c})

    g_q[c, z, x] = wq_in[...]
    acc[...] = jnp.zeros_like(acc)
    stat[:, 0] = jnp.full((2, 8, 256), LOW, F32)
    stat[:, 1] = jnp.zeros((2, 8, 256), F32)
    pl.semaphore_wait(barrier, 17 - jnp.where(o_self, 2, 0) - jnp.where(y_to == y, 2, 0))

    r_land, r_o = book.slot(2), book.slot(1)
    pos = (x, z, c)
    gq = Plane(book, g_q, pos, 4, 3)
    gx = Plane(book, g_x, pos, 3, 4)
    go = Plane(book, g_o, pos, 4, 3)

    gq.x_send()

    def to_or_own(src, dst, recv_at, device, own):
        book.start(src, dst, recv_at, device, jnp.logical_not(own))

        @pl.when(own)
        def _():
            pltpu.make_async_copy(src, dst, recv_sem.at[recv_at]).start()

    for j in (0, 1):
        own = (y_to == y) & (h == j)
        for hh in (0, 1):
            here = h == hh
            book.start(wx_in, land.at[hh], r_land + hh, {"tp_0": y_to, "tp_1": j}, here & jnp.logical_not(own))

            @pl.when(here & own)
            def _():
                pltpu.make_async_copy(wx_in, land.at[hh], recv_sem.at[r_land + hh]).start()
    o_slot = g_o.at[c, y, 2 * h + lax.rem(z, 2)]
    to_or_own(wo_in, o_slot, r_o, xzyh(o_to), o_self)

    gq.x_wait()
    book.wait(land.at[0], r_land)
    book.wait(land.at[1], r_land + 1)
    lane = lax.broadcasted_iota(jnp.int32, (56, HD), 1)
    g_x[c, z, x] = jnp.where(lane < 64, land[0].astype(F32), land[1].astype(F32)).astype(BF16)
    gx.x_send()
    gq.step(1)
    gx.x_wait()
    gq.step(2)
    gx.step(1)
    gq.step(3)
    gx.step(2)
    gq.step(4)
    gx.step(3)
    gx.step(4)
    book.wait(g_o.at[c, z, x], r_o)
    go.x_send()

    def assemble(g, w):
        def one(i, carry):
            xx, zz = lax.div(i, NZ), lax.rem(i, NZ)
            both = jnp.concatenate([g[0, zz, xx].astype(F32), g[1, zz, xx].astype(F32)], axis=0)
            w[i] = both.astype(BF16)
            return carry

        lax.fori_loop(0, NX * NZ, one, 0)

    r_q = book.slot(1)
    gq.core_wait()
    assemble(g_q, w_q)
    q_sum = jnp.dot(hid[...], w_q[...].reshape(3584, HD), preferred_element_type=F32)
    qq[p] = (q_sum * (HD ** -0.5)).astype(BF16)
    book.start(qq.at[p], qq.at[p], r_q, {"tp_0": y2})
    gx.core_wait()
    assemble(g_x, w_x)
    x_sum = jnp.dot(hid[...], w_x[...].reshape(3584, HD), preferred_element_type=F32)

    halves = x_sum.reshape(2, HD, HD)
    turned = jnp.stack([halves[0].T, halves[1].T])
    block = jnp.where(p == 0, halves, turned).astype(BF16)
    moves = c != p
    mine = kv.at[c, z, 0]

    @pl.when(moves)
    def _():
        made[...] = block

    @pl.when(jnp.logical_not(moves))
    def _():
        kv[c, z, 0] = block

    r_pair = book.slot(1)
    book.start(made, kv.at[p, z, 0], r_pair, {"tp_0": y2, "dp_2": 1 - c}, moves)
    book.wait(mine, r_pair, moves)

    n_steps = 4
    r_xk = book.slot(2)
    r_ring = {(s, k, r): book.slot(1) for s in (1, -1) for k in range(1, 5) for r in range(3)}
    r_cx = book.slot(3)
    r_cring = {(s, k, r): book.slot(1) for s in (1, -1) for k in range(1, 5) for r in range(3)}
    r_far, r_cfar = book.slot(1), book.slot(1)

    far_from = (x == 0) & (z == 7) & (p == 1)
    far_to = (x == 3) & (z == 0) & (p == 1)
    far = kv.at[c, NZ, 0]
    for d in (1, 2):
        book.start(mine, kv.at[c, z, d], r_xk + d - 1, {"dp_0": wrap(x + d, NX)}, x + d <= 3)
    book.start(mine, far, r_far, {"dp_0": 3 - x, "dp_1": 7 - z}, far_from)

    def ring(k, rows, step):
        for r in rows:
            to = wrap(z + step, NZ)
            pred = received(step, k, r, to)
            if pred is not None:
                ref = kv.at[c, wrap(z - step * (k - 1), NZ), r]
                book.start(ref, ref, r_ring[step, k, r], {"dp_1": to}, pred & (x >= r))

    def to_core(ref, at, pred):
        book.start(ref, ref, at, {"dp_2": 1 - c}, pred)

    for s in (1, -1):
        ring(1, (0,), s)
    to_core(mine, r_cx, None)
    for d in (1, 2):
        book.wait(kv.at[c, z, d], r_xk + d - 1, x >= d)
        for s in (1, -1):
            ring(1, (d,), s)
        to_core(kv.at[c, z, d], r_cx + d, x >= d)

    book.wait(qq.at[1 - p], r_q)
    q_pos = (2 * (x * NZ + z) + c) * 256 + lax.broadcasted_iota(jnp.int32, (1, 256), 1)
    q_low = qstart[...]

    def attend(zz, row, chunk):
        keys = kv[0, zz, row].reshape(256, HD)
        k_pos = (2 * chunk + p) * 256 + lax.broadcasted_iota(jnp.int32, (256, 256), 0)
        allowed = (k_pos >= q_low) & (k_pos <= q_pos)
        for hd in (0, 1):
            scores = lax.dot_general(keys, qq[hd], (((1,), (1,)), ((), ())), preferred_element_type=F32)
            scores = jnp.where(allowed, scores, LOW)
            old = stat[hd, 0, 0:1]
            new = jnp.maximum(old, jnp.max(scores, axis=0, keepdims=True))
            expw = jnp.where(allowed, jnp.exp(scores - new), 0.0)
            scale = jnp.exp(old - new)
            stat[hd, 1] = stat[hd, 1] * scale + jnp.sum(expw, axis=0, keepdims=True)
            stat[hd, 0] = jnp.broadcast_to(new, (8, 256))
            probs = expw.astype(BF16)
            numer = jnp.dot(kv[1, zz, row, 0], probs[:HD], preferred_element_type=F32)
            numer = numer + jnp.dot(kv[1, zz, row, 1], probs[HD:], preferred_element_type=F32)
            acc[hd] = acc[hd] * scale + numer

    def attend_some(preds, place):
        def one(i, carry):
            on = i < 0
            for n, pred in enumerate(preds):
                if pred is not None:
                    on = on | ((i == n) & pred)

            @pl.when(on)
            def _():
                zz, row = place(i)
                attend(zz, row, (x - row) * NZ + zz)

            return carry

        lax.fori_loop(0, len(preds), one, 0)

    def attend_own():
        for d in (0, 1, 2):
            book.wait(kv.at[1 - c, z, d], r_cx + d, None if d == 0 else x >= d)
        attend_some([x >= 0, x >= 1, x >= 2], lambda i: (z, i))

    def attend_step(k):
        preds = []
        for s in (1, -1):
            for r in range(3):
                need = needed(s, k, r, z)
                if need is not None:
                    need = need & (x >= r)
                    book.wait(kv.at[1 - c, wrap(z - s * k, NZ), r], r_cring[s, k, r], need)
                preds.append(need)
        attend_some(preds, lambda i: (wrap(z - k + 2 * k * lax.div(i, 3), NZ), lax.rem(i, 3)))

    for k in range(1, n_steps + 1):
        for s in (1, -1):
            for r in range(3):
                got = received(s, k, r, z)
                if got is None:
                    continue
                ref = kv.at[c, wrap(z - s * k, NZ), r]
                book.wait(ref, r_ring[s, k, r], got & (x >= r))
                if k < n_steps:
                    ring(k + 1, (r,), s)
                to_core(ref, r_cring[s, k, r], needed(s, k, r, z) & (x >= r))
        if k == 3:
            go.x_wait()
        if k == 4:
            go.step(1)
        if k == 1:
            book.wait(far, r_far, far_to)
            to_core(far, r_cfar, far_to)
            attend_own()
        else:
            attend_step(k - 1)
    go.step(2)
    attend_step(4)
    book.wait(kv.at[1 - c, NZ, 0], r_cfar, far_to)

    @pl.when(far_to)
    def _():
        attend(NZ, 0, 7)

    r_acc, r_stat = book.slot(1), book.slot(1)
    book.start(stat.at[1 - p], stat_in, r_stat, {"tp_0": y2})
    book.start(acc.at[1 - p], o_in, r_acc, {"tp_0": y2})
    go.step(3)
    book.wait(stat_in, r_stat)
    book.wait(o_in, r_acc)
    m_a, m_b = stat[p, 0, 0:1], stat_in[0, 0:1]
    top = jnp.maximum(m_a, m_b)
    e_a, e_b = jnp.exp(m_a - top), jnp.exp(m_b - top)
    denom = stat[p, 1, 0:1] * e_a + stat_in[1, 0:1] * e_b
    heads[y, h] = ((acc[p] * e_a + o_in[...] * e_b) / denom).astype(BF16)

    r_h = book.slot(1)
    r_head = [{(s, k): book.slot(1) for s in (1, -1) for k in range(1, 5)} for _ in range(2)]
    last = ({1: 4, -1: 3}, {1: 3, -1: 4})
    own_heads = heads.at[y, h]
    book.start(own_heads, own_heads, r_h, {"tp_1": 1 - h})

    def head_hop(which, k, s):
        ref = heads.at[wrap(y - s * (k - 1), NY), h if which == 0 else 1 - h]
        book.start(ref, ref, r_head[which][s, k], {"tp_0": wrap(y + s, NY)})

    def head_step(which, k):
        for s in (1, -1):
            if k <= last[which][s]:
                book.wait(heads.at[wrap(y - s * k, NY), h if which == 0 else 1 - h], r_head[which][s, k])
                if k < last[which][s]:
                    head_hop(which, k + 1, s)

    for s in (1, -1):
        head_hop(0, 1, s)
    go.step(4)
    head_step(0, 1)
    go.core_wait()

    def weights(t, carry):
        yy, hh = lax.div(t, 2), lax.rem(t, 2)
        parts = [g_o[cc, yy, 2 * hh + b].astype(F32) for b in (0, 1) for cc in (0, 1)]
        w_t[t] = jnp.concatenate(parts, axis=0).astype(BF16)
        return carry

    lax.fori_loop(0, NY * NH, weights, 0)
    book.wait(heads.at[y, 1 - h], r_h)
    for s in (1, -1):
        head_hop(1, 1, s)
    for k in (1, 2, 3):
        head_step(0, k + 1)
        head_step(1, k)
    head_step(1, 4)

    total[...] = jnp.zeros_like(total)

    def group(t, carry):
        yy, hh = lax.div(t, 2), lax.rem(t, 2)
        term = jnp.dot(w_t[t], heads[yy, hh], preferred_element_type=F32).astype(BF16)
        total[0:224] = total[0:224] + term.astype(F32)
        return carry

    lax.fori_loop(0, NY * NH, group, 0)
    out[...] = total[...].T[:, :224].astype(BF16)
    book.finish()


def body(hidden_states, resp_lengths, w_query, w_keyval, w_out):
    rows = hidden_states.shape[0]
    ends = jnp.cumsum(resp_lengths, dtype=jnp.int32)
    q_pos = lax.axis_index(DP) * rows + jnp.arange(rows, dtype=jnp.int32)
    begun = jnp.where(q_pos[None, :] >= ends[:, None], ends[:, None], 0)
    q_start = jnp.max(begun, axis=0)[None, :]
    wx = jnp.concatenate([w_keyval, w_keyval], axis=1)
    wo = w_out.T
    vmem = pl.BlockSpec(memory_space=pltpu.VMEM)
    return pl.pallas_call(
        kernel,
        out_shape=jax.ShapeDtypeStruct((rows, 224), BF16),
        in_specs=[vmem] * 5,
        out_specs=vmem,
        scratch_shapes=[
            pltpu.VMEM((NC, NZ, NX, 56, HD), BF16),
            pltpu.VMEM((NC, NZ, NX, 56, HD), BF16),
            pltpu.VMEM((NC, NZ, NX, 56, HD), BF16),
            pltpu.VMEM((2, 56, HD), BF16),
            pltpu.VMEM((NX * NZ, 112, HD), BF16),
            pltpu.VMEM((NX * NZ, 112, HD), BF16),
            pltpu.VMEM((16, 224, HD), BF16),
            pltpu.VMEM((2, 256, HD), BF16),
            pltpu.VMEM((2, HD, HD), BF16),
            pltpu.VMEM((2, NZ + 1, 3, 2, HD, HD), BF16),
            pltpu.VMEM((2, HD, 256), F32),
            pltpu.VMEM((2, 2, 8, 256), F32),
            pltpu.VMEM((HD, 256), F32),
            pltpu.VMEM((2, 8, 256), F32),
            pltpu.VMEM((NY, NH, HD, 256), BF16),
            pltpu.VMEM((256, 256), F32),
            pltpu.SemaphoreType.DMA((160,)),
            pltpu.SemaphoreType.DMA((160,)),
        ],
        compiler_params=pltpu.CompilerParams(
            collective_id=0, has_side_effects=True, vmem_limit_bytes=48 * 1024 * 1024),
        name="layer",
    )(hidden_states, q_start, w_query, wx, wo)


def solution(mesh):
    finer = Mesh(mesh.devices.reshape(4, 8, 2, 8, 2), (*DP, *TP))
    placed = (P(DP, None), P(), P(DP, TP), P(DP, TP), P(TP, DP))
    return jax.shard_map(body, mesh=finer, in_specs=placed, out_specs=P(DP, TP), check_vma=False)
```

```python
import functools

import jax
import jax.numpy as jnp
from jax import lax
from jax.experimental import pallas as pl
from jax.experimental.pallas import tpu as pltpu
from jax.sharding import Mesh
from jax.sharding import PartitionSpec as P

HD = 128
DP = ("dp_0", "dp_1", "dp_2")
TP = ("tp_0", "tp_1")
MESH = pl.DeviceIdType.MESH
F32, BF16 = jnp.float32, jnp.bfloat16
NX, NZ, NC, NY, NH = 4, 8, 2, 8, 2
LOW = -1e30


def wrap(a, n):
    return lax.rem(a + 2 * n, n)


class Book:
    def __init__(self, send, recv):
        self.send, self.recv, self.n_recv, self.open = send, recv, 0, []
        self.free = list(range(send.shape[0]))

    def slot(self, count=1):
        at = self.n_recv
        self.n_recv += count
        return at

    def start(self, src, dst, recv_at, device, pred=None):
        if not self.free:
            self.settle()
        at = self.free.pop(0)
        copy = pltpu.make_async_remote_copy(
            src_ref=src, dst_ref=dst, send_sem=self.send.at[at], recv_sem=self.recv.at[recv_at],
            device_id=device, device_id_type=MESH)
        self.open.append((copy, pred, at))
        if pred is None:
            copy.start()
        else:
            pl.when(pred)(copy.start)

    def wait(self, dst, recv_at, pred=None):
        copy = pltpu.make_async_remote_copy(
            src_ref=dst, dst_ref=dst, send_sem=self.send.at[0], recv_sem=self.recv.at[recv_at],
            device_id={"dp_2": 1 - lax.axis_index("dp_2")}, device_id_type=MESH)
        if pred is None:
            copy.wait_recv()
        else:
            pl.when(pred)(copy.wait_recv)

    def settle(self):
        copy, pred, at = self.open.pop(0)
        if pred is None:
            copy.wait_send()
        else:
            pl.when(pred)(copy.wait_send)
        self.free.append(at)

    def finish(self):
        while self.open:
            self.settle()


class Plane:
    def __init__(self, book, buf, pos, up, down, parts, late):
        self.book, self.buf, self.parts = book, buf, parts
        self.x, self.z, self.c = pos
        self.last = {1: up, -1: down}
        self.rx = book.slot()
        self.rz = {(s, k): book.slot(parts) for s in (1, -1) for k in range(1, self.last[s] + 1)}
        self.late, self.rcore = late, book.slot(1 + late)

    def core(self, k, zz):
        ref = self.buf.at[self.c, zz]
        self.book.start(ref, ref, self.rcore + (1 if self.late and k == 4 else 0), {"dp_2": 1 - self.c})

    def x_send(self):
        ref = self.buf.at[self.c, self.z, self.x]
        for d in (1, 2, 3):
            self.book.start(ref, ref, self.rx, {"dp_0": wrap(self.x + d, NX)})

    def slab(self, zz, part):
        size = NX // self.parts
        return self.buf.at[self.c, zz, pl.ds(part * size, size)]

    def hop(self, k, step, part):
        ref = self.slab(wrap(self.z - step * (k - 1), NZ), part)
        self.book.start(ref, ref, self.rz[step, k] + part, {"dp_1": wrap(self.z + step, NZ)})

    def x_wait(self):
        self.book.wait(self.buf.at[self.c, self.z, pl.ds(0, NX - 1)], self.rx)

    def begin(self):
        for part in range(self.parts):
            self.hop(1, 1, part)
            self.hop(1, -1, part)
        self.core(0, self.z)

    def step(self, k):
        steps = [s for s in (1, -1) if k <= self.last[s]]
        for part in range(self.parts):
            for s in steps:
                self.book.wait(self.slab(wrap(self.z - s * k, NZ), part), self.rz[s, k] + part)
                if k < self.last[s]:
                    self.hop(k + 1, s, part)
        for s in steps:
            self.core(k, wrap(self.z - s * k, NZ))

    def core_wait(self, last=False):
        theirs = self.buf.at[1 - self.c]
        if last:
            self.book.wait(theirs.at[0], self.rcore + 1)
        else:
            self.book.wait(theirs.at[pl.ds(0, NZ - 1)] if self.late else theirs, self.rcore)


def received(step, k, row, z):
    if step == 1:
        if row == 0:
            return z >= k
        if row == 1:
            return None if k > 4 else (z >= 0 if k <= 3 else z < 4)
        if k == 1:
            return z >= 0
        if k == 2:
            return (z <= 1) | (z == 7)
        return z <= 2 if k == 3 else None
    if row == 2:
        return z <= 7 - k
    if row == 1:
        return z >= 0 if k <= 3 else z >= 4
    if k == 1:
        return (z == 7) | (z <= 1)
    if k == 2:
        return (z >= 6) | (z == 0)
    return z >= 5 if k == 3 else None


def needed(step, k, row, z):
    if row == 1:
        return received(step, k, row, z)
    if row == 0:
        return (z >= k) if step == 1 else (None if k > 3 else z + k >= 8)
    if step == -1:
        return z <= 7 - k
    if k == 1:
        return z >= 0
    return z < k if k <= 3 else None


def kernel(lengths, hid_in, wq_in, wkv_in, wo_in, out,
           hid, wkv, wx, wo, g_q, g_x, g_o, land, w_q, w_x, w_t, qq, made, kv, acc, stat,
           o_out, o_in, stat_in, heads, total, local_sem, send_sem, recv_sem):
    x, z, c = (lax.axis_index(a) for a in DP)
    y, h = (lax.axis_index(a) for a in TP)
    p = lax.rem(y, 2)
    y2 = y + 1 - 2 * p
    book = Book(send_sem, recv_sem)
    fetches = [pltpu.make_async_copy(src, dst, local_sem.at[n]) for n, (src, dst) in enumerate((
        (wkv_in, wkv), (wq_in, g_q.at[c, z, x]), (wo_in, wo), (hid_in, hid)))]
    for fetch in fetches:
        fetch.start()

    y_to = lax.rem(2 * y, NY) + lax.div(y, 4)
    y_from = lax.div(y, 2) + 4 * p
    o_to = (2 * h + lax.rem(z, 2), y, 2 * x + lax.div(z, 4), lax.rem(lax.div(z, 2), 2))
    o_from = (lax.div(y, 2), 4 * p + 2 * h + lax.rem(x, 2), z, lax.div(x, 2))

    def xzyh(t):
        return {"dp_0": t[0], "dp_1": t[1], "tp_0": t[2], "tp_1": t[3]}

    o_self = (o_to[0] == x) & (o_to[1] == z) & (o_to[2] == y) & (o_to[3] == h)
    barrier = pltpu.get_barrier_semaphore()

    def greet(device, own=None):
        def remote():
            pl.semaphore_signal(barrier, inc=1, device_id=device, device_id_type=MESH)

        if own is None:
            remote()
        else:
            pl.when(jnp.logical_not(own))(remote)

    greet(xzyh(o_to), o_self)
    greet(xzyh(o_from), o_self)
    for d in range(NX):
        for j in (0, 1):
            device = {"dp_0": wrap(x + d, NX), "tp_1": j}
            own = (y_to == y) & (h == j) if d == 0 else None
            greet({**device, "tp_0": y_to}, own)
            greet({**device, "tp_0": y_from}, own)
    greet({"dp_0": 3 - x, "dp_1": 7 - z})
    greet({"tp_1": 1 - h})
    for d in (1, 2, 3):
        greet({"dp_0": wrap(x + d, NX)})
    for d in (1, -1):
        greet({"dp_1": wrap(z + d, NZ)})
        greet({"tp_0": wrap(y + d, NY)})
    for d in range(NX):
        greet({"dp_0": wrap(x + d, NX), "tp_0": y2, "dp_2": 1 - c})
    greet({"dp_2": 1 - c})

    acc[...] = jnp.zeros_like(acc)
    stat[:, 0] = jnp.full((2, 8, 256), LOW, F32)
    stat[:, 1] = jnp.zeros((2, 8, 256), F32)
    fetches[0].wait()
    pair = wkv[...].astype(F32)
    wx[...] = jnp.concatenate([pair, pair], axis=1).astype(BF16)
    fetches[1].wait()
    pl.semaphore_wait(barrier, 32 - jnp.where(o_self, 2, 0) - jnp.where(y_to == y, 2, 0))

    r_land, r_o = book.slot(1), book.slot(1)
    pos = (x, z, c)
    gq = Plane(book, g_q, pos, 4, 3, 2, 0)
    gx = Plane(book, g_x, pos, 3, 4, 2, 1)
    go = Plane(book, g_o, pos, 4, 3, 1, 0)

    def to_or_own(src, dst, recv_at, device, own):
        book.start(src, dst, recv_at, device, jnp.logical_not(own))

        @pl.when(own)
        def _():
            pltpu.make_async_copy(src, dst, recv_sem.at[recv_at]).start()

    for d in range(NX):
        for j in (0, 1):
            device = {"dp_0": wrap(x + d, NX), "tp_0": y_to, "tp_1": j}
            if d == 0:
                to_or_own(wx, land.at[x, h], r_land, device, (y_to == y) & (h == j))
            else:
                book.start(wx, land.at[x, h], r_land, device)
    gq.x_send()

    gq.x_wait()
    gq.begin()
    lane = lax.broadcasted_iota(jnp.int32, (56, HD), 1)
    book.wait(land, r_land)
    for xx in range(NX):
        g_x[c, z, xx] = jnp.where(lane < 64, land[xx, 0].astype(F32), land[xx, 1].astype(F32)).astype(BF16)
    gx.begin()
    fetches[2].wait()
    to_or_own(wo, g_o.at[c, y, 2 * h + lax.rem(z, 2)], r_o, xzyh(o_to), o_self)

    def assemble(g, w, first, count):
        def one(i, carry):
            zz, xx = wrap(z + first + lax.div(i, NX), NZ), lax.rem(i, NX)
            both = jnp.concatenate([g[0, zz, xx].astype(F32), g[1, zz, xx].astype(F32)], axis=0)
            w[xx * NZ + zz] = both.astype(BF16)
            return carry

        lax.fori_loop(0, NX * count, one, 0)

    gq.step(1)
    gx.step(1)
    gq.step(2)
    gx.step(2)
    gq.step(3)
    gx.step(3)
    gq.step(4)
    gq.core_wait()
    assemble(g_q, w_q, 0, NZ)
    fetches[3].wait()
    r_q = book.slot(1)
    q_sum = jnp.dot(hid[...], w_q[...].reshape(3584, HD), preferred_element_type=F32)
    qq[p] = (q_sum * (HD ** -0.5)).astype(BF16)
    gx.core_wait()
    assemble(g_x, w_x, -3, NZ - 1)
    gx.step(4)
    gx.core_wait(True)
    assemble(g_x, w_x, 4, 1)
    x_sum = jnp.dot(hid[...], w_x[...].reshape(3584, HD), preferred_element_type=F32)

    halves = x_sum.reshape(2, HD, HD)
    turned = jnp.stack([halves[0].T, halves[1].T])
    block = jnp.where(p == 0, halves, turned).astype(BF16)
    moves = c != p
    mine = kv.at[c, z, 0]

    @pl.when(moves)
    def _():
        made[...] = block

    @pl.when(jnp.logical_not(moves))
    def _():
        kv[c, z, 0] = block

    r_pair = book.slot(1)
    r_xk = book.slot(2)
    for d in (0, 1, 2):
        fits = x + d <= 3
        book.start(made, kv.at[p, z, d], r_pair if d == 0 else r_xk + d - 1,
                   {"dp_0": wrap(x + d, NX), "tp_0": y2, "dp_2": 1 - c}, moves & fits)
        if d > 0:
            book.start(mine, kv.at[c, z, d], r_xk + d - 1, {"dp_0": wrap(x + d, NX)}, jnp.logical_not(moves) & fits)
    book.start(qq.at[p], qq.at[p], r_q, {"tp_0": y2})
    book.wait(mine, r_pair, moves)

    n_steps = 4
    hops = [(s, k, r) for s in (1, -1) for k in range(1, 5) for r in range(3) if received(s, k, r, z) is not None]
    r_ring = {hop: book.slot(2) for hop in hops}
    r_cx = book.slot(3)
    r_cring = {hop: book.slot(1) for hop in hops}
    r_far, r_cfar = book.slot(1), book.slot(1)

    far_from = (x == 0) & (z == 7) & (p == 1)
    far_to = (x == 3) & (z == 0) & (p == 1)
    far = kv.at[c, NZ, 0]
    book.start(mine, far, r_far, {"dp_0": 3 - x, "dp_1": 7 - z}, far_from)

    def ring(k, r, step, half):
        if (step, k, r) in r_ring:
            to = wrap(z + step, NZ)
            ref = kv.at[c, wrap(z - step * (k - 1), NZ), r, half]
            pred = received(step, k, r, to) & (x >= r)
            book.start(ref, ref, r_ring[step, k, r] + half, {"dp_1": to}, pred)

    def to_core(ref, at, pred):
        book.start(ref, ref, at, {"dp_2": 1 - c}, pred)

    def ring_start(r):
        for half in (0, 1):
            for s in (1, -1):
                ring(1, r, s, half)

    ring_start(0)
    to_core(mine, r_cx, None)
    for d in (1, 2):
        book.wait(kv.at[c, z, d], r_xk + d - 1, x >= d)
        ring_start(d)
        to_core(kv.at[c, z, d], r_cx + d, x >= d)

    book.wait(qq.at[1 - p], r_q)
    q_pos = (2 * (x * NZ + z) + c) * 256 + lax.broadcasted_iota(jnp.int32, (1, 256), 1)
    q_low, end = jnp.zeros((1, 256), jnp.int32), jnp.int32(0)
    for n in range(lengths.shape[0]):
        end = end + lengths[n]
        q_low = jnp.where(q_pos >= end, end, q_low)

    def attend(zz, row, chunk):
        keys = kv[0, zz, row].reshape(256, HD)
        k_pos = (2 * chunk + p) * 256 + lax.broadcasted_iota(jnp.int32, (256, 256), 0)
        allowed = (k_pos >= q_low) & (k_pos <= q_pos)
        for hd in (0, 1):
            scores = lax.dot_general(keys, qq[hd], (((1,), (1,)), ((), ())), preferred_element_type=F32)
            scores = jnp.where(allowed, scores, LOW)
            old = stat[hd, 0, 0:1]
            new = jnp.maximum(old, jnp.max(scores, axis=0, keepdims=True))
            expw = jnp.where(allowed, jnp.exp(scores - new), 0.0)
            scale = jnp.exp(old - new)
            stat[hd, 1] = stat[hd, 1] * scale + jnp.sum(expw, axis=0, keepdims=True)
            stat[hd, 0] = jnp.broadcast_to(new, (8, 256))
            probs = expw.astype(BF16)
            numer = jnp.dot(kv[1, zz, row, 0], probs[:HD], preferred_element_type=F32)
            numer = numer + jnp.dot(kv[1, zz, row, 1], probs[HD:], preferred_element_type=F32)
            acc[hd] = acc[hd] * scale + numer

    def attend_some(preds, place):
        def one(i, carry):
            on = i < 0
            for n, pred in enumerate(preds):
                if pred is not None:
                    on = on | ((i == n) & pred)

            @pl.when(on)
            def _():
                zz, row = place(i)
                attend(zz, row, (x - row) * NZ + zz)

            return carry

        lax.fori_loop(0, len(preds), one, 0)

    def attend_own():
        for d in (0, 1, 2):
            book.wait(kv.at[1 - c, z, d], r_cx + d, None if d == 0 else x >= d)
        attend_some([x >= 0, x >= 1, x >= 2], lambda i: (z, i))

    def attend_step(k):
        preds = []
        for s in (1, -1):
            for r in range(3):
                need = needed(s, k, r, z)
                if need is not None:
                    need = need & (x >= r)
                    book.wait(kv.at[1 - c, wrap(z - s * k, NZ), r], r_cring[s, k, r], need)
                preds.append(need)
        attend_some(preds, lambda i: (wrap(z - k + 2 * k * lax.div(i, 3), NZ), lax.rem(i, 3)))

    for k in range(1, n_steps + 1):
        for r in range(3):
            steps = [s for s in (1, -1) if (s, k, r) in r_ring]
            for half in (0, 1):
                for s in steps:
                    ref = kv.at[c, wrap(z - s * k, NZ), r, half]
                    book.wait(ref, r_ring[s, k, r] + half, received(s, k, r, z) & (x >= r))
                    ring(k + 1, r, s, half)
            for s in steps:
                to_core(kv.at[c, wrap(z - s * k, NZ), r], r_cring[s, k, r], needed(s, k, r, z) & (x >= r))
        if k == 1:
            book.wait(far, r_far, far_to)
            to_core(far, r_cfar, far_to)
            book.wait(g_o.at[c, z, x], r_o)
            go.x_send()
            attend_own()
        else:
            attend_step(k - 1)
        if k == 3:
            go.x_wait()
        if k == 4:
            go.begin()
    attend_step(4)
    book.wait(kv.at[1 - c, NZ, 0], r_cfar, far_to)

    @pl.when(far_to)
    def _():
        attend(NZ, 0, 7)

    r_acc, r_stat = book.slot(1), book.slot(1)
    o_out[...] = acc[1 - p].astype(BF16)
    book.start(stat.at[1 - p], stat_in, r_stat, {"tp_0": y2})
    book.start(o_out, o_in, r_acc, {"tp_0": y2})
    total[...] = jnp.zeros_like(total)
    book.wait(stat_in, r_stat)
    m_a, m_b = stat[p, 0, 0:1], stat_in[0, 0:1]
    top = jnp.maximum(m_a, m_b)
    e_a, e_b = jnp.exp(m_a - top), jnp.exp(m_b - top)
    denom = stat[p, 1, 0:1] * e_a + stat_in[1, 0:1] * e_b
    book.wait(o_in, r_acc)
    merged = ((acc[p] * e_a + o_in[...].astype(F32) * e_b) / denom).astype(BF16)
    heads[y, h, 0] = merged[:, :HD]
    heads[y, h, 1] = merged[:, HD:]

    r_h = book.slot(2)
    last = ({1: 4, -1: 3}, {1: 3, -1: 4})
    r_head = [{(s, k): book.slot(2) for s in (1, -1) for k in range(1, ends[s] + 1)} for ends in last]
    side = (h, 1 - h)

    def head_hop(which, k, s, half):
        ref = heads.at[wrap(y - s * (k - 1), NY), side[which], half]
        book.start(ref, ref, r_head[which][s, k] + half, {"tp_0": wrap(y + s, NY)})

    def head_step(which, k):
        for half in (0, 1):
            for s in (1, -1):
                if k <= last[which][s]:
                    book.wait(heads.at[wrap(y - s * k, NY), side[which], half], r_head[which][s, k] + half)
                    if k < last[which][s]:
                        head_hop(which, k + 1, s, half)

    for half in (0, 1):
        own = heads.at[y, h, half]
        book.start(own, own, r_h + half, {"tp_1": 1 - h})
        for s in (1, -1):
            head_hop(0, 1, s, half)

    def add_group(yy, hh):
        values = jnp.concatenate([heads[yy, hh, 0], heads[yy, hh, 1]], axis=1)
        term = jnp.dot(w_t[2 * yy + hh], values, preferred_element_type=F32).astype(BF16)
        total[...] = total[...] + term.astype(F32)

    def weights(t, carry):
        yy, hh = lax.div(t, 2), lax.rem(t, 2)
        parts = [g_o[cc, yy, 2 * hh + b].astype(F32) for b in (0, 1) for cc in (0, 1)]
        w_t[t] = jnp.concatenate(parts, axis=0).astype(BF16)
        return carry

    def add_step(which, k):
        steps = [1] if k == 0 else [s for s in (1, -1) if k <= last[which][s]]

        def one(i, carry):
            add_group(wrap(y - k + 2 * k * i, NY) if steps[0] == 1 else wrap(y + k, NY), side[which])
            return carry

        lax.fori_loop(0, len(steps), one, 0)

    go.step(1)
    head_step(0, 1)
    for half in (0, 1):
        book.wait(heads.at[y, 1 - h, half], r_h + half)
        for s in (1, -1):
            head_hop(1, 1, s, half)
    go.step(2)
    head_step(0, 2)
    head_step(1, 1)
    go.step(3)
    head_step(0, 3)
    head_step(1, 2)
    go.step(4)
    head_step(0, 4)
    go.core_wait()
    lax.fori_loop(0, NY * NH, weights, 0)
    add_step(0, 0)
    add_step(1, 0)
    add_step(0, 1)
    add_step(1, 1)
    head_step(1, 3)
    for k in (2, 3):
        add_step(0, k)
    add_step(0, 4)
    for k in (2, 3):
        add_step(1, k)
    head_step(1, 4)
    add_step(1, 4)
    out[...] = total[...].astype(BF16)
    book.finish()


def body(hidden_states, resp_lengths, w_query, w_keyval, w_out):
    rows = hidden_states.shape[0]
    vmem, hbm = pl.BlockSpec(memory_space=pltpu.VMEM), pl.BlockSpec(memory_space=pl.ANY)
    return pl.pallas_call(
        kernel,
        out_shape=jax.ShapeDtypeStruct((224, rows), BF16),
        in_specs=[pl.BlockSpec(memory_space=pltpu.SMEM)] + [hbm] * 4,
        out_specs=vmem,
        scratch_shapes=[
            pltpu.VMEM((256, 3584), BF16),
            pltpu.VMEM((56, 64), BF16),
            pltpu.VMEM((56, HD), BF16),
            pltpu.VMEM((56, HD), BF16),
            pltpu.VMEM((NC, NZ, NX, 56, HD), BF16),
            pltpu.VMEM((NC, NZ, NX, 56, HD), BF16),
            pltpu.VMEM((NC, NZ, NX, 56, HD), BF16),
            pltpu.VMEM((NX, NH, 56, HD), BF16),
            pltpu.VMEM((NX * NZ, 112, HD), BF16),
            pltpu.VMEM((NX * NZ, 112, HD), BF16),
            pltpu.VMEM((16, 224, HD), BF16),
            pltpu.VMEM((2, 256, HD), BF16),
            pltpu.VMEM((2, HD, HD), BF16),
            pltpu.VMEM((2, NZ + 1, 3, 2, HD, HD), BF16),
            pltpu.VMEM((2, HD, 256), F32),
            pltpu.VMEM((2, 2, 8, 256), F32),
            pltpu.VMEM((HD, 256), BF16),
            pltpu.VMEM((HD, 256), BF16),
            pltpu.VMEM((2, 8, 256), F32),
            pltpu.VMEM((NY, NH, 2, HD, HD), BF16),
            pltpu.VMEM((224, 256), F32),
            pltpu.SemaphoreType.DMA((4,)),
            pltpu.SemaphoreType.DMA((40,)),
            pltpu.SemaphoreType.DMA((151,)),
        ],
        compiler_params=pltpu.CompilerParams(
            collective_id=0, has_side_effects=True, vmem_limit_bytes=60 * 1024 * 1024),
        name="layer",
    )(resp_lengths, hidden_states, w_query, w_keyval, w_out.T).T


def solution(mesh):
    finer = Mesh(mesh.devices.reshape(4, 8, 2, 8, 2), (*DP, *TP))
    placed = (P(DP, None), P(), P(DP, TP), P(DP, TP), P(TP, DP))
    return jax.shard_map(body, mesh=finer, in_specs=placed, out_specs=P(DP, TP), check_vma=False)
```
